32 devices in a mesh: front: 2 (over core), row: 4 (over y, x), col: 4 (over z).
Axes of the slice: x: 2, y: 2, z: 4, core: 2. Of those that a mesh axis runs over, the one named last changes fastest.
Arguments:
- front_rows: float32 [4096, 24576], P(('front', 'row'), 'col'), parts along dimension 0, may hold values from -0.0546875 to 0.0546875
- random_columns: bfloat16 [49152, 512], P(('front', 'col'), 'row'), parts along dimension 0, may hold values from -6 to 6
Outputs:
- basis: float32 [4096, 256], P(('front', 'row', 'col')), parts along dimension 0
- projected: float32 [1024, 512], P(('front', 'row')), parts along dimension 0
The draws below stay inside these ranges and needn't reach their ends.
There are 2 independent parts, one for each index of `front`. The reference program is written for one: setup_inputs(seed, part) draws one part's arguments, and reference() takes and returns one part's arrays. A program takes and returns all parts, laid end to end along the dimension named above; each array names one. Nothing has to cross between parts.
All inputs are finite; a program needn't handle non-finite values.
Results may differ from the reference program's by a relative error of at most 0.0003.
Values may be sent and summed in bfloat16 or wider, within the bound.
A program may use at most 64 MiB of HBM per device.

```python
import jax
import jax.numpy as jnp
from jax import lax

ORDER = 24576
SAMPLES = 512
LEAF = 1024
RANK = 256
ROWS = 2048


def raised(entries, own_key, source, target, blocks, factor):
    owner, partner = [(jnp.arange(entries.shape[position]) // (entries.shape[position] // blocks)).reshape([-1 if axis == position else 1 for axis in range(entries.ndim)]) for position in (source, target)]
    chosen = jax.random.permutation(own_key, blocks)[partner]
    strong = (owner == chosen) | (owner == (partner + blocks // 2) % blocks)
    return jnp.where(strong, factor * entries, entries)


def steps_of(stream_key, shape, shards, least, top_value):
    factor_of = 1.0
    for axis_at, parts in shards:
        heights = jax.random.uniform(jax.random.fold_in(jax.random.fold_in(stream_key, 6), axis_at), (parts,), jnp.float32, least / len(shards), top_value / len(shards))
        factor_of = factor_of * jnp.repeat(jnp.exp(heights), shape[axis_at] // parts).reshape((-1,) + (1,) * (len(shape) - 1 - axis_at))
    return factor_of


def centred(stream_key, extent, deviation, bound, shards=(), kind=jnp.bfloat16):
    factor_of = steps_of(stream_key, extent, shards, -0.22, 0.18) if shards else 1.0
    array = jax.random.normal(stream_key, extent, jnp.float32) * deviation * factor_of
    return jnp.minimum(jnp.maximum(array, -bound), bound).astype(kind)


def bell_draw_with(rng, dims, deviation, most, pieces, heavy, kind=jnp.bfloat16):
    drawn = deviation * jax.random.normal(rng, dims, jnp.float32)
    if pieces:
        drawn = drawn * steps_of(rng, dims, pieces, -0.22, 0.18)
    return jnp.clip(raised(drawn, jax.random.fold_in(rng, 3), *heavy), -most, most).astype(kind)


def setup_inputs(seed: int = 0, part: int = 0) -> dict:
    seeds = jax.random.split(jax.random.key(seed), 3)
    part_keys = jax.random.split(jax.random.fold_in(seeds[2], part), 3)
    front_rows = bell_draw_with(part_keys[0], (ROWS, ORDER), ORDER ** -0.5, 0.0546875, ((0, 4), (1, 4)), (1, 0, 4, 2.0), jnp.float32)
    random_columns = centred(part_keys[1], (ORDER, SAMPLES), 1.0, 6.0, ((0, 4), (1, 4)))
    return {"front_rows": front_rows, "random_columns": random_columns}


def reference(front_rows, random_columns):
    sketch = jnp.dot(front_rows.astype(jnp.float32), random_columns.astype(jnp.float32), precision=lax.Precision.HIGHEST, preferred_element_type=jnp.float32)
    count = ROWS // LEAF
    blocks = sketch.reshape(count, LEAF, SAMPLES)
    factor_q, factor_r = jnp.linalg.qr(blocks)
    diagonal = jnp.diagonal(factor_r, axis1=1, axis2=2)
    signs = jnp.where(diagonal < 0, -1.0, 1.0).astype(factor_r.dtype)
    factor_q = factor_q * signs[:, None, :]
    factor_r = factor_r * signs[:, :, None]
    basis = factor_q[:, :, :RANK].reshape(count * LEAF, RANK)
    projected = factor_r[:, :RANK, :].reshape(count * RANK, SAMPLES)
    return (basis, projected)
```

```python
import functools

import jax
import jax.numpy as jnp
from jax import lax
from jax.experimental import pallas as pl
from jax.experimental.pallas import tpu as pltpu
from jax.sharding import PartitionSpec as P

RANK = 256
PANEL = 8
MESH = pl.DeviceIdType.MESH

OUT_X = (
    ((0, 0), (1, 0), (0, 1), (0, 0)),
    ((2, 1), (3, 1), (1, 0), (1, 1)),
    ((3, 0), (2, 0), (2, 0), (3, 0)),
)
OUT_Y = (
    ((0, 1), (0, 0), (2, 1), (0, 1)),
    ((1, 0), (1, 1), (1, 1), (3, 1)),
    ((3, 1), (2, 1), (3, 0), (2, 0)),
)
RELAY_X = ((0, 0, 1, 1), (0, 1, 1, 1), (1, 1, 0, 0))
RELAY_Y = ((0, 1, 0, 1), (0, 0, 1, 0), (0, 0, 1, 1))
ROUNDS = len(OUT_X)


def product(left, right, contract):
    return lax.dot_general(
        left,
        right,
        ((contract[:1], contract[1:]), ((), ())),
        precision=lax.Precision.HIGHEST,
        preferred_element_type=jnp.float32,
    )


def lookup(table, x, y):
    a, b, c, d = table
    return a + (b - a) * x + (c - a) * y + (a + d - b - c) * x * y


def factor(block, work):
    size = block.shape[0]
    rows = lax.broadcasted_iota(jnp.int32, (size, size), 0)
    lanes = lax.broadcasted_iota(jnp.int32, (size, size), 1)
    work[:, :size] = block
    work[:, size:] = jnp.where(rows == lanes, 1.0, 0.0).astype(jnp.float32)
    row_of = lax.broadcasted_iota(jnp.int32, (PANEL, 1), 0)
    for start in range(0, size, PANEL):
        panel = work[start : start + PANEL, :]
        for step in range(PANEL):
            column = panel[:, start + step : start + step + 1]
            scale = lax.rsqrt(column[step : step + 1, :])
            pivot = panel[step : step + 1, :] * scale
            weight = jnp.where(row_of > step, column * scale, 0.0)
            panel = jnp.where(row_of == step, pivot, panel - weight * pivot)
        work[start : start + PANEL, :] = panel
        if start + PANEL < size:
            tall = jnp.transpose(panel[:, :size])
            rest = work[start + PANEL :, :]
            for step in range(PANEL):
                rest = rest - tall[start + PANEL :, step : step + 1] * panel[step : step + 1, :]
            work[start + PANEL :, :] = rest
    return jnp.where(rows <= lanes, work[:, :size], 0.0), work[:, size:]


def kernel(
    cols,
    a_ref,
    om_ref,
    basis_ref,
    projected_ref,
    a32,
    high,
    low,
    om,
    part,
    rs_buf,
    sketch,
    gram,
    gram_in,
    t_own,
    t_in,
    t_sum,
    tr_buf,
    t_all,
    work,
    a_sem,
    om_sem,
    ring_send,
    ring_recv,
    rs_send,
    rs_recv,
    ag_send,
    ag_recv,
    g_send,
    g_recv,
    t_send,
    t_recv,
):
    _, chunks, depth, width = om_ref.shape
    ahead = min(2, (chunks - 1) // 4)
    own_rows = part.shape[1] // cols
    half = RANK // 2
    front, row, col = lax.axis_index("front"), lax.axis_index("row"), lax.axis_index("col")
    x, y = lax.rem(row, 2), lax.div(row, 2)
    beside = (front, row + 1 - 2 * x, col)
    above = (front, row + 2 - 4 * y, col)

    def along(step):
        return (front, row, lax.rem(col + step, cols))

    own_load = pltpu.make_async_copy(om_ref, om.at[pl.ds(2 * row, 2)], om_sem)
    own_load.start()

    def a_load(j):
        columns = pl.ds(pl.multiple_of(j * depth, depth), depth)
        return pltpu.make_async_copy(a_ref.at[:, columns], a32.at[j], a_sem.at[j])

    for i in range(chunks):
        for h in range(2):
            a_load(h * chunks + i).start()

    barrier = pltpu.get_barrier_semaphore()
    peers = [beside, above] + [along(step) for step in range(1, cols)]
    for peer in peers:
        pl.semaphore_signal(barrier, inc=1, device_id=peer, device_id_type=MESH)
    part[...] = jnp.zeros_like(part)
    own_load.wait()
    pl.semaphore_wait(barrier, len(peers))

    total_steps = ROUNDS * chunks + 4 * ahead
    lags = (
        ahead * lookup((3, 0, 2, 1), x, y),
        ahead * lookup((3, 2, 0, 1), x, y),
    )
    late = 4 * ahead * x * (1 - y)
    out_lag = ahead * x * y

    def pick(values, number):
        first, second, third = values
        middle = number * (2 - number)
        last = lax.div(number * (number - 1), 2)
        return first + (second - first) * middle + (third - first) * last

    def flipped(axis):
        return (1 - x, y) if axis == 0 else (x, 1 - y)

    def slots(axis, px, py):
        table = (OUT_X, OUT_Y)[axis]
        return [
            lookup([2 * block + side for block, side in entry], px, py)
            for entry in table
        ]

    leaving = [slots(axis, x, y) for axis in (0, 1)]
    coming = [slots(axis, *flipped(axis)) for axis in (0, 1)]
    relays = [
        [lookup(entry, x, y) for entry in table] for table in (RELAY_X, RELAY_Y)
    ]

    def hop(number, axis, i, slot):
        return pltpu.make_async_remote_copy(
            src_ref=om.at[slot, i],
            dst_ref=om.at[slot, i],
            send_sem=ring_send.at[number, axis, i],
            recv_sem=ring_recv.at[number, axis, i],
            device_id=(beside, above)[axis],
            device_id_type=MESH,
        )

    def accumulate(slot, i):
        block = lax.div(slot, 2)
        j = lax.rem(slot, 2) * chunks + i
        columns = om[slot, i]
        part[block] += jnp.dot(
            high[j], columns, preferred_element_type=jnp.float32
        ) + jnp.dot(low[j], columns, preferred_element_type=jnp.float32)

    def step_of(g, convert):
        found = []
        for axis in (0, 1):
            at = g - lags[axis]
            third = lax.div(at, 2 * chunks)
            at = at - late * third if axis == 0 else at
            live = jnp.logical_and(at >= 2 * chunks * third, at < ROUNDS * chunks)
            live = jnp.logical_and(g >= lags[axis], live)
            number = lax.div(at, chunks)
            i = lax.rem(at, chunks)
            slot = pick(coming[axis], number)
            relay = pick(relays[1 - axis], number)
            found.append((live, slot, i))

            @pl.when(live)
            def _():
                hop(number, axis, i, slot).wait_recv()

                @pl.when(relay == 1)
                def _():
                    hop(number, 1 - axis, i, slot).start()

        for axis in (0, 1):
            at = g + 1 - out_lag
            number = lax.div(at, chunks)
            i = lax.rem(at, chunks)
            relay = pick(relays[axis], number)
            due = jnp.logical_and(at >= chunks, at < ROUNDS * chunks)

            @pl.when(jnp.logical_and(due, relay == 0))
            def _():
                hop(number, axis, i, pick(leaving[axis], number)).start()

        if convert:
            for h in range(2):
                j = h * chunks + g
                a_load(j).wait()
                value = a32[j]
                near = value.astype(jnp.bfloat16)
                high[j] = near
                low[j] = (value - near.astype(jnp.float32)).astype(jnp.bfloat16)
            for h in range(2):
                accumulate(2 * row + h, g)
        for live, slot, i in found:

            @pl.when(live)
            def _():
                accumulate(slot, i)

    def launch():
        for axis in (0, 1):

            @pl.when(relays[axis][0] == 0)
            def _():
                @pl.loop(0, chunks)
                def _(i):
                    hop(0, axis, i, leaving[axis][0]).start()

    def gather(hooks):
        marks = sorted(set(hooks) | {chunks, total_steps})
        begin = 0
        for mark in marks:
            pl.loop(begin, mark)(functools.partial(step_of, convert=mark <= chunks))
            if mark in hooks:
                hooks[mark]()
            begin = mark

    def scatter(s, step):
        target = lax.rem(col + step, cols)
        rows = pl.ds(pl.multiple_of(target * own_rows, own_rows), own_rows)
        return pltpu.make_async_remote_copy(
            src_ref=part.at[s, rows],
            dst_ref=rs_buf.at[s, step - 1],
            send_sem=rs_send.at[s, step - 1],
            recv_sem=rs_recv.at[s, step - 1],
            device_id=along(step),
            device_id_type=MESH,
        )

    def spread(s, step, piece):
        return pltpu.make_async_remote_copy(
            src_ref=sketch.at[s, piece],
            dst_ref=sketch.at[s, piece],
            send_sem=ag_send.at[s, step - 1],
            recv_sem=ag_recv.at[s, step - 1],
            device_id=along(step),
            device_id_type=MESH,
        )

    def scatter_start(s):
        for step in range(1, cols):
            scatter(s, step).start()

    def scatter_end(s):
        rows = pl.ds(pl.multiple_of(col * own_rows, own_rows), own_rows)
        total = part[s, rows]
        for step in range(1, cols):
            scatter(s, step).wait_recv()
            total = total + rs_buf[s, step - 1]
        sketch[s, col] = total
        for step in range(1, cols):
            spread(s, step, col).start()

    def spread_end(s):
        for step in range(1, cols):
            spread(s, step, lax.rem(col + cols - step, cols)).wait_recv()
        return sketch[s].reshape(part.shape[1], width)

    def exchange(first, count):
        return pltpu.make_async_remote_copy(
            src_ref=gram.at[pl.ds(first, count)],
            dst_ref=gram_in.at[pl.ds(first, count)],
            send_sem=g_send.at[first],
            recv_sem=g_recv.at[first],
            device_id=beside,
            device_id_type=MESH,
        )

    def first_done():
        scatter_start(1)
        value = spread_end(0)
        gram[0] = product(value, value, (0, 0))
        exchange(0, 1).start()

    ready = chunks + 2 * ahead
    ready_next = 2 * chunks + 3 * ahead
    launch()
    gather({
        ready: lambda: scatter_start(0),
        (ready + ready_next) // 2: lambda: scatter_end(0),
        ready_next: first_done,
        min(ready_next + 7, total_steps): lambda: scatter_end(1),
    })

    first = sketch[0].reshape(part.shape[1], width)
    second = spread_end(1)
    gram[1] = product(first, second, (0, 0))
    gram[2] = product(second, second, (0, 0))
    exchange(1, 2).start()
    exchange(0, 1).wait_recv()
    upper_a, inverse_a = factor(gram[0] + gram_in[0], work)
    q_a = product(first, inverse_a, (1, 1))
    exchange(1, 2).wait_recv()
    across = product(inverse_a, gram[1] + gram_in[1], (1, 0))
    rest = second - product(q_a, across, (1, 0))
    for s in range(2):
        columns = slice(s * width, (s + 1) * width)
        t_own[0, :, columns] = product(q_a, part[2 + s], (0, 0))
        t_own[1, :, columns] = product(rest, part[2 + s], (0, 0))

    swap = pltpu.make_async_remote_copy(
        src_ref=t_own.at[1 - x],
        dst_ref=t_in,
        send_sem=t_send.at[0, 0],
        recv_sem=t_recv.at[0, 0],
        device_id=beside,
        device_id_type=MESH,
    )
    swap.start()
    schur = gram[2] + gram_in[2] - product(across, across, (0, 0))
    swap.wait_recv()
    t_rows = half // cols
    t_sum[...] = (t_own[x] + t_in[...]).reshape(t_sum.shape)

    def t_scatter(step):
        return pltpu.make_async_remote_copy(
            src_ref=t_sum.at[lax.rem(col + step, cols)],
            dst_ref=tr_buf.at[step - 1],
            send_sem=t_send.at[1, step - 1],
            recv_sem=t_recv.at[1, step - 1],
            device_id=along(step),
            device_id_type=MESH,
        )

    def t_spread(step, piece):
        return pltpu.make_async_remote_copy(
            src_ref=t_all.at[piece],
            dst_ref=t_all.at[piece],
            send_sem=t_send.at[2, step - 1],
            recv_sem=t_recv.at[2, step - 1],
            device_id=along(step),
            device_id_type=MESH,
        )

    for step in range(1, cols):
        t_scatter(step).start()
    total = t_sum[col]
    for step in range(1, cols):
        t_scatter(step).wait_recv()
        total = total + tr_buf[step - 1]
    t_all[col] = total
    for step in range(1, cols):
        t_spread(step, col).start()

    upper_b, inverse_b = factor(schur, work)
    mine_a = product(sketch[0, col], inverse_a, (1, 1))
    basis_ref[:, :half] = mine_a
    mine_b = sketch[1, col] - product(mine_a, across, (1, 0))
    basis_ref[:, half:] = product(mine_b, inverse_b, (1, 1))

    for step in range(1, cols):
        t_spread(step, lax.rem(col + cols - step, cols)).wait_recv()
    tail = t_all[...].reshape(half, 2 * width)
    is_low = x == 0
    projected_ref[:, :half] = jnp.where(is_low, upper_a, 0.0)
    projected_ref[:, half:RANK] = jnp.where(is_low, across, upper_b)
    projected_ref[:, RANK:] = jnp.where(is_low, tail, product(inverse_b, tail, (1, 0)))

    for number in range(ROUNDS):
        for axis in (0, 1):

            @pl.loop(0, chunks)
            def _(i):
                hop(number, axis, i, leaving[axis][number]).wait_send()

    for step in range(1, cols):
        for s in range(2):
            scatter(s, step).wait_send()
            spread(s, step, col).wait_send()
        t_scatter(step).wait_send()
        t_spread(step, col).wait_send()
    exchange(0, 1).wait_send()
    exchange(1, 2).wait_send()
    swap.wait_send()


def per_device(front_rows, random_columns):
    block_rows, depth = front_rows.shape
    width = random_columns.shape[1]
    cols = lax.axis_size("col")
    half = RANK // 2
    own_rows = block_rows // cols
    chunk = 256 if depth >= 4096 else 128
    chunks = depth // 2 // chunk
    columns = random_columns.reshape(2, chunks, chunk, width)
    vmem = pltpu.VMEM
    f32, bf16 = jnp.float32, jnp.bfloat16
    dma = pltpu.SemaphoreType.DMA
    return pl.pallas_call(
        functools.partial(kernel, cols),
        out_shape=(
            jax.ShapeDtypeStruct((own_rows, RANK), f32),
            jax.ShapeDtypeStruct((half, 4 * width), f32),
        ),
        in_specs=[pl.BlockSpec(memory_space=pl.ANY)] * 2,
        out_specs=(pl.BlockSpec(memory_space=pltpu.VMEM),) * 2,
        scratch_shapes=[
            vmem((2 * chunks, block_rows, chunk), f32),
            vmem((2 * chunks, block_rows, chunk), bf16),
            vmem((2 * chunks, block_rows, chunk), bf16),
            vmem((8, chunks, chunk, width), bf16),
            vmem((4, block_rows, width), f32),
            vmem((2, cols - 1, own_rows, width), f32),
            vmem((2, cols, own_rows, width), f32),
            vmem((3, half, half), f32),
            vmem((3, half, half), f32),
            vmem((2, half, 2 * width), f32),
            vmem((half, 2 * width), f32),
            vmem((cols, half // cols, 2 * width), f32),
            vmem((cols - 1, half // cols, 2 * width), f32),
            vmem((cols, half // cols, 2 * width), f32),
            vmem((half, RANK), f32),
            dma((2 * chunks,)),
            dma,
            dma((ROUNDS, 2, chunks)),
            dma((ROUNDS, 2, chunks)),
            dma((2, cols - 1)),
            dma((2, cols - 1)),
            dma((2, cols - 1)),
            dma((2, cols - 1)),
            dma((2,)),
            dma((2,)),
            dma((3, cols - 1)),
            dma((3, cols - 1)),
        ],
        compiler_params=pltpu.CompilerParams(
            collective_id=0, has_side_effects=True, vmem_limit_bytes=60 << 20
        ),
    )(front_rows, columns)


def solution(mesh):
    return jax.shard_map(
        per_device,
        mesh=mesh,
        in_specs=(P(("front", "row"), "col"), P(("front", "col"), "row")),
        out_specs=(P(("front", "row", "col"), None), P(("front", "row"), None)),
        check_vma=False,
    )
```

```python
import functools

import jax
import jax.numpy as jnp
from jax import lax
from jax.experimental import pallas as pl
from jax.experimental.pallas import tpu as pltpu
from jax.sharding import PartitionSpec as P

RANK = 256
PANEL = 8
CHUNK = 256
LAG = 3
FACTOR_LAG = 4
MESH = pl.DeviceIdType.MESH


def send_plan(size, lag):
    n, d = size, lag
    x_runs = (
        ((0, n, 0, 0), (n, n, 5, 0), (2 * n, 2 * d, 6, 0), (2 * n + 4 * d, n - 3 * d, 6, 2 * d)),
        (
            (0, n, 2, 0),
            (n, 2 * d, 7, 0),
            (n + 2 * d, d, 3, n - d),
            (n + 3 * d, n - 2 * d, 7, 2 * d),
            (2 * n + d, d, 4, 0),
            (2 * n + 3 * d, n - 2 * d, 4, d),
        ),
        ((0, d, 4, 0), (d, n, 1, 0), (n + d, n, 2, 0), (2 * n + d, n - d, 4, d)),
        ((0, 2 * d, 6, 0), (2 * d, n, 0, 0), (n + 2 * d, n, 3, 0), (2 * n + 2 * d, n - 2 * d, 6, 2 * d)),
    )
    y_runs = (
        ((0, n, 1, 0), (n, n, 2, 0), (2 * n, n, 7, 0)),
        ((0, d, 3, 0), (d, n, 0, 0), (n + d, n - d, 3, d), (2 * n, n, 5, 0)),
        (
            (0, n, 5, 0),
            (n, 2 * d, 6, 0),
            (n + 3 * d, n - d, 3, 0),
            (2 * n + 2 * d, d, 4, n - d),
            (2 * n + 3 * d, n - 2 * d, 6, 2 * d),
        ),
        (
            (0, 2 * d, 7, 0),
            (2 * d, n, 1, 0),
            (n + 2 * d, n - 2 * d, 7, 2 * d),
            (2 * n, d, 4, 0),
            (2 * n + d, d, 6, n - d),
            (2 * n + 2 * d, n - d, 4, d),
        ),
    )
    taken = [{(2 * row + h, i): 0 for h in range(2) for i in range(n)} for row in range(4)]
    for axis, runs_of in enumerate((x_runs, y_runs)):
        for row, runs in enumerate(runs_of):
            for start, length, slot, chunk in runs:
                for i in range(length):
                    taken[row ^ (1, 2)[axis]][slot, chunk + i] = start + i + d
    plan = []
    for runs_of in (x_runs, y_runs):
        most = max(len(runs) for runs in runs_of)
        table = []
        for row, runs in enumerate(runs_of):
            sent, free, rows = 0, 0, []
            for start, length, slot, chunk in runs:
                ready = [taken[row][slot, chunk + i] for i in range(length)]
                at_once = max([free] + ready)
                stream = max([free] + [when - i for i, when in enumerate(ready)])
                if at_once <= stream or at_once <= start:
                    issue, free = (at_once, 0, 0), at_once
                else:
                    issue, free = (-1, stream, stream + length), stream + length - 1
                rows.append(
                    (start, start + length, slot, chunk - start, sent - start, chunk, sent, length)
                    + issue
                )
                sent += length
            rows += [(0,) * 8 + (-1, 0, 0)] * (most - len(runs))
            table.append((rows, sent))
        plan.append(table)
    return plan


def product(left, right, contract):
    return lax.dot_general(
        left,
        right,
        ((contract[:1], contract[1:]), ((), ())),
        precision=lax.Precision.HIGHEST,
        preferred_element_type=jnp.float32,
    )


def lookup(table, x, y):
    a, b, c, d = table
    return a + (b - a) * x + (c - a) * y + (a + d - b - c) * x * y


def factor(block, work):
    size = block.shape[0]
    rows = lax.broadcasted_iota(jnp.int32, (size, size), 0)
    lanes = lax.broadcasted_iota(jnp.int32, (size, size), 1)
    work[:, :size] = block
    work[:, size:] = jnp.where(rows == lanes, 1.0, 0.0).astype(jnp.float32)
    row_of = lax.broadcasted_iota(jnp.int32, (PANEL, 1), 0)
    for start in range(0, size, PANEL):
        panel = work[start : start + PANEL, :]
        for step in range(PANEL):
            column = panel[:, start + step : start + step + 1]
            scale = lax.rsqrt(column[step : step + 1, :])
            pivot = panel[step : step + 1, :] * scale
            weight = jnp.where(row_of > step, column * scale, 0.0)
            panel = jnp.where(row_of == step, pivot, panel - weight * pivot)
        work[start : start + PANEL, :] = panel
        if start + PANEL < size:
            tall = jnp.transpose(panel[:, :size])
            rest = work[start + PANEL :, :]
            for step in range(PANEL):
                rest = rest - tall[start + PANEL :, step : step + 1] * panel[step : step + 1, :]
            work[start + PANEL :, :] = rest
        yield


def factored(work):
    size = work.shape[0]
    rows = lax.broadcasted_iota(jnp.int32, (size, size), 0)
    lanes = lax.broadcasted_iota(jnp.int32, (size, size), 1)
    return jnp.where(rows <= lanes, work[:, :size], 0.0), work[:, size:]


def kernel(
    cols,
    lag,
    a_ref,
    om_ref,
    basis_ref,
    projected_ref,
    a32,
    high,
    low,
    om,
    part,
    rs_buf,
    sketch,
    gram,
    gram_in,
    t_own,
    t_in,
    t_sum,
    tr_buf,
    t_all,
    work_a,
    work_b,
    a_sem,
    om_sem,
    ring_send,
    ring_recv,
    rs_send,
    rs_recv,
    ag_send,
    ag_recv,
    g_send,
    g_recv,
    t_send,
    t_recv,
):
    _, chunks, depth, width = om_ref.shape
    own_rows = part.shape[1] // cols
    half = RANK // 2
    front, row, col = lax.axis_index("front"), lax.axis_index("row"), lax.axis_index("col")
    x, y = lax.rem(row, 2), lax.div(row, 2)
    beside = (front, row + 1 - 2 * x, col)
    above = (front, row + 2 - 4 * y, col)

    def along(step):
        return (front, row, lax.rem(col + step, cols))

    upper = lax.div(2 * col, cols)
    outward = [step + upper * (cols - 2 * step) for step in range(cols - 1, 0, -1)]

    own_load = pltpu.make_async_copy(om_ref, om.at[pl.ds(2 * row, 2)], om_sem)
    own_load.start()

    def a_load(j):
        columns = pl.ds(pl.multiple_of(j * depth, depth), depth)
        return pltpu.make_async_copy(a_ref.at[:, columns], a32.at[j], a_sem.at[j])

    for i in range(chunks):
        for h in range(2):
            a_load(h * chunks + i).start()

    barrier = pltpu.get_barrier_semaphore()
    peers = [beside, above] + [along(step) for step in range(1, cols)]
    for peer in peers:
        pl.semaphore_signal(barrier, inc=1, device_id=peer, device_id_type=MESH)
    part[...] = jnp.zeros_like(part)
    own_load.wait()
    pl.semaphore_wait(barrier, len(peers))

    plan = send_plan(chunks, lag)
    total_steps = 3 * chunks + 2 * lag

    def runs_at(axis, px, py):
        table = plan[axis]
        return [
            [lookup([rows[k][field] for rows, _ in table], px, py) for field in range(11)]
            for k in range(len(table[0][0]))
        ]

    leaving = [runs_at(axis, x, y) for axis in (0, 1)]
    coming = [runs_at(0, 1 - x, y), runs_at(1, x, 1 - y)]

    def chosen(runs, at):
        live, slot, i, order = False, 0, 0, 0
        for start, end, run_slot, run_chunk, run_order, *_ in runs:
            inside = jnp.logical_and(at >= start, at < end)
            live = jnp.logical_or(live, inside)
            slot = jnp.where(inside, run_slot, slot)
            i = jnp.where(inside, run_chunk + at, i)
            order = jnp.where(inside, run_order + at, order)
        return live, slot, i, order

    def hop(axis, slot, i, order):
        return pltpu.make_async_remote_copy(
            src_ref=om.at[slot, i],
            dst_ref=om.at[slot, i],
            send_sem=ring_send.at[axis, order],
            recv_sem=ring_recv.at[axis, order],
            device_id=(beside, above)[axis],
            device_id_type=MESH,
        )

    def accumulate(slot, i):
        block = lax.div(slot, 2)
        j = lax.rem(slot, 2) * chunks + i
        columns = om[slot, i]
        part[block] += jnp.dot(
            high[j], columns, preferred_element_type=jnp.float32
        ) + jnp.dot(low[j], columns, preferred_element_type=jnp.float32)

    def issue(axis, g):
        for k, run in enumerate(leaving[axis]):
            _, _, slot, _, _, chunk, sent, length, at_once, stream, stop = run
            if any(rows[k][8] >= 0 for rows, _ in plan[axis]):

                @pl.when(at_once == g)
                def _():
                    @pl.loop(0, length)
                    def _(i):
                        hop(axis, slot, chunk + i, sent + i).start()

            if any(rows[k][10] > 0 for rows, _ in plan[axis]):

                @pl.when(jnp.logical_and(g >= stream, g < stop))
                def _():
                    i = g - stream
                    hop(axis, slot, chunk + i, sent + i).start()

    def step_of(g, convert):
        found = []
        for axis in (0, 1):
            live, slot, i, order = chosen(coming[axis], g - lag)
            found.append((live, slot, i))

            @pl.when(live)
            def _():
                hop(axis, slot, i, order).wait_recv()

            issue(1 - axis, g)

        if convert:
            for h in range(2):
                j = h * chunks + g
                a_load(j).wait()
                value = a32[j]
                near = value.astype(jnp.bfloat16)
                high[j] = near
                low[j] = (value - near.astype(jnp.float32)).astype(jnp.bfloat16)
            for h in range(2):
                accumulate(2 * row + h, g)
        for live, slot, i in found:

            @pl.when(live)
            def _():
                accumulate(slot, i)

    def gather(hooks):
        marks = sorted(set(hooks) | {chunks, total_steps})
        begin = 0
        for mark in marks:
            if mark > begin + 1:
                pl.loop(begin, mark)(functools.partial(step_of, convert=mark <= chunks))
            elif mark > begin:
                step_of(begin, convert=mark <= chunks)
            for hook in hooks.get(mark, ()):
                hook()
            begin = mark

    def scatter(s, step):
        target = lax.rem(col + step, cols)
        rows = pl.ds(pl.multiple_of(target * own_rows, own_rows), own_rows)
        return pltpu.make_async_remote_copy(
            src_ref=part.at[s, rows],
            dst_ref=rs_buf.at[s, step - 1],
            send_sem=rs_send.at[s, step - 1],
            recv_sem=rs_recv.at[s, step - 1],
            device_id=along(step),
            device_id_type=MESH,
        )

    def spread(s, step, piece):
        return pltpu.make_async_remote_copy(
            src_ref=sketch.at[s, piece],
            dst_ref=sketch.at[s, piece],
            send_sem=ag_send.at[s, step - 1],
            recv_sem=ag_recv.at[s, step - 1],
            device_id=along(step),
            device_id_type=MESH,
        )

    def scatter_start(s):
        for step in outward:
            scatter(s, step).start()

    def scatter_end(s):
        rows = pl.ds(pl.multiple_of(col * own_rows, own_rows), own_rows)
        total = part[s, rows]
        for step in range(1, cols):
            scatter(s, step).wait_recv()
            total = total + rs_buf[s, step - 1]
        sketch[s, col] = total
        for step in outward:
            spread(s, step, col).start()

    def spread_end(s):
        for step in range(1, cols):
            spread(s, step, lax.rem(col + cols - step, cols)).wait_recv()
        return sketch[s].reshape(part.shape[1], width)

    def exchange(first, count):
        return pltpu.make_async_remote_copy(
            src_ref=gram.at[pl.ds(first, count)],
            dst_ref=gram_in.at[pl.ds(first, count)],
            send_sem=g_send.at[first],
            recv_sem=g_recv.at[first],
            device_id=beside,
            device_id_type=MESH,
        )

    factor_a = []

    def first_done():
        value = spread_end(0)
        gram[0] = product(value, value, (0, 0))
        exchange(0, 1).start()

    def first_panel():
        exchange(0, 1).wait_recv()
        factor_a.append(factor(gram[0] + gram_in[0], work_a))
        next(factor_a[0])

    def next_panel():
        for _ in range(per_step):
            next(factor_a[0], None)

    ready = chunks + 3 * lag
    ready_next = 2 * chunks + 3 * lag
    panel_step = min(ready_next + FACTOR_LAG, total_steps - 1)
    panels = half // PANEL
    per_step = -(-panels // (total_steps - panel_step))
    hooks = {}
    for at, hook in (
        (ready, lambda: scatter_start(0)),
        ((ready + ready_next) // 2, lambda: scatter_end(0)),
        (ready_next, lambda: scatter_start(1)),
        (ready_next, first_done),
        (min(ready_next + chunks // 2, total_steps), lambda: scatter_end(1)),
        (panel_step, first_panel),
    ):
        hooks.setdefault(at, []).append(hook)
    for at in range(panel_step + 1, total_steps + 1):
        hooks.setdefault(at, []).append(next_panel)
    gather(hooks)
    for _ in factor_a[0]:
        pass

    first = sketch[0].reshape(part.shape[1], width)
    upper_a, inverse_a = factored(work_a)
    q_a = product(first, inverse_a, (1, 1))

    def projection(left):
        return jnp.concatenate(
            [product(left, part[2 + s], (0, 0)) for s in range(2)], axis=1
        )

    t_own[0] = projection(q_a)
    second = spread_end(1)
    gram[1] = product(first, second, (0, 0))
    exchange(1, 1).start()
    gram[2] = product(second, second, (0, 0))
    exchange(2, 1).start()
    coarse = projection(second)
    mine_a = product(sketch[0, col], inverse_a, (1, 1))
    basis_ref[:, :half] = mine_a
    exchange(1, 1).wait_recv()
    across = product(inverse_a, gram[1] + gram_in[1], (1, 0))
    t_own[1] = coarse - product(across, t_own[0], (0, 0))

    swap = pltpu.make_async_remote_copy(
        src_ref=t_own.at[1 - x],
        dst_ref=t_in,
        send_sem=t_send.at[0, 0],
        recv_sem=t_recv.at[0, 0],
        device_id=beside,
        device_id_type=MESH,
    )
    swap.start()
    exchange(2, 1).wait_recv()
    schur = gram[2] + gram_in[2] - product(across, across, (0, 0))
    factor_b = factor(schur, work_b)
    for _ in range(panels * 7 // 16):
        next(factor_b)
    swap.wait_recv()
    t_sum[...] = (t_own[x] + t_in[...]).reshape(t_sum.shape)

    def t_scatter(step):
        return pltpu.make_async_remote_copy(
            src_ref=t_sum.at[lax.rem(col + step, cols)],
            dst_ref=tr_buf.at[step - 1],
            send_sem=t_send.at[1, step - 1],
            recv_sem=t_recv.at[1, step - 1],
            device_id=along(step),
            device_id_type=MESH,
        )

    def t_spread(step, piece):
        return pltpu.make_async_remote_copy(
            src_ref=t_all.at[piece],
            dst_ref=t_all.at[piece],
            send_sem=t_send.at[2, step - 1],
            recv_sem=t_recv.at[2, step - 1],
            device_id=along(step),
            device_id_type=MESH,
        )

    for step in outward:
        t_scatter(step).start()
    for _ in factor_b:
        pass
    total = t_sum[col]
    for step in range(1, cols):
        t_scatter(step).wait_recv()
        total = total + tr_buf[step - 1]
    t_all[col] = total
    for step in outward:
        t_spread(step, col).start()

    upper_b, inverse_b = factored(work_b)
    mine_b = sketch[1, col] - product(mine_a, across, (1, 0))
    basis_ref[:, half:] = product(mine_b, inverse_b, (1, 1))

    for step in range(1, cols):
        t_spread(step, lax.rem(col + cols - step, cols)).wait_recv()
    tail = t_all[...].reshape(half, 2 * width)
    is_low = x == 0
    projected_ref[:, :half] = jnp.where(is_low, upper_a, 0.0)
    projected_ref[:, half:RANK] = jnp.where(is_low, across, upper_b)
    projected_ref[:, RANK:] = jnp.where(is_low, tail, product(inverse_b, tail, (1, 0)))

    for axis in (0, 1):

        @pl.loop(0, lookup([sent for _, sent in plan[axis]], x, y))
        def _(order):
            hop(axis, 0, 0, order).wait_send()

    for step in range(1, cols):
        for s in range(2):
            scatter(s, step).wait_send()
            spread(s, step, col).wait_send()
        t_scatter(step).wait_send()
        t_spread(step, col).wait_send()
    exchange(0, 1).wait_send()
    exchange(1, 1).wait_send()
    exchange(2, 1).wait_send()
    swap.wait_send()


def per_device(front_rows, random_columns):
    block_rows, depth = front_rows.shape
    width = random_columns.shape[1]
    cols = lax.axis_size("col")
    half = RANK // 2
    own_rows = block_rows // cols
    chunk = min(CHUNK, depth // 12 // 128 * 128)
    chunks = depth // 2 // chunk
    lag = max(1, min(LAG, chunks // 4))
    columns = random_columns.reshape(2, chunks, chunk, width)
    vmem = pltpu.VMEM
    f32, bf16 = jnp.float32, jnp.bfloat16
    dma = pltpu.SemaphoreType.DMA
    return pl.pallas_call(
        functools.partial(kernel, cols, lag),
        out_shape=(
            jax.ShapeDtypeStruct((own_rows, RANK), f32),
            jax.ShapeDtypeStruct((half, 4 * width), f32),
        ),
        in_specs=[pl.BlockSpec(memory_space=pl.ANY)] * 2,
        out_specs=(pl.BlockSpec(memory_space=pltpu.VMEM),) * 2,
        scratch_shapes=[
            vmem((2 * chunks, block_rows, chunk), f32),
            vmem((2 * chunks, block_rows, chunk), bf16),
            vmem((2 * chunks, block_rows, chunk), bf16),
            vmem((8, chunks, chunk, width), bf16),
            vmem((4, block_rows, width), f32),
            vmem((2, cols - 1, own_rows, width), f32),
            vmem((2, cols, own_rows, width), f32),
            vmem((3, half, half), f32),
            vmem((3, half, half), f32),
            vmem((2, half, 2 * width), f32),
            vmem((half, 2 * width), f32),
            vmem((cols, half // cols, 2 * width), f32),
            vmem((cols - 1, half // cols, 2 * width), f32),
            vmem((cols, half // cols, 2 * width), f32),
            vmem((half, RANK), f32),
            vmem((half, RANK), f32),
            dma((2 * chunks,)),
            dma,
            dma((2, 3 * chunks + lag)),
            dma((2, 3 * chunks + lag)),
            dma((2, cols - 1)),
            dma((2, cols - 1)),
            dma((2, cols - 1)),
            dma((2, cols - 1)),
            dma((3,)),
            dma((3,)),
            dma((3, cols - 1)),
            dma((3, cols - 1)),
        ],
        compiler_params=pltpu.CompilerParams(
            collective_id=0, has_side_effects=True, vmem_limit_bytes=60 << 20
        ),
    )(front_rows, columns)


def solution(mesh):
    return jax.shard_map(
        per_device,
        mesh=mesh,
        in_specs=(P(("front", "row"), "col"), P(("front", "col"), "row")),
        out_specs=(P(("front", "row", "col"), None), P(("front", "row"), None)),
        check_vma=False,
    )
```

```python
import functools

import jax
import jax.numpy as jnp
from jax import lax
from jax.experimental import pallas as pl
from jax.experimental.pallas import tpu as pltpu
from jax.sharding import PartitionSpec as P

RANK = 256
PANEL = 8
CHUNK = 256
LAG = 3
SUM_LAG = 6
FACTOR_LAG = 3
PANELS_A_STEP = 4
MESH = pl.DeviceIdType.MESH


def send_plan(size, lag):
    n, d = size, lag
    x_runs = (
        ((0, n, 0, 0), (n, n, 5, 0), (2 * n, n, 4, 0)),
        ((0, n, 2, 0), (n, n, 3, 0), (2 * n, n, 7, 0)),
        ((0, d, 4, 0), (d, n, 1, 0), (n + d, n, 2, 0), (2 * n + d, n - d, 4, d)),
        (
            (0, 2 * d, 6, 0),
            (2 * d, n, 0, 0),
            (n + 2 * d, n - d, 3, 0),
            (2 * n + d, n - 2 * d, 6, 2 * d),
            (3 * n - d, d, 7, n - d),
        ),
    )
    y_runs = (
        ((0, n, 1, 0), (n, n, 2, 0), (2 * n, d, 3, n - d), (2 * n + d, n - d, 7, 0)),
        ((0, d, 3, 0), (d, n, 0, 0), (n + d, n - d, 3, d), (2 * n, n, 5, 0)),
        ((0, n, 5, 0), (n, n, 4, 0), (2 * n, 2 * d, 6, 0), (2 * n + 2 * d, n - 2 * d, 6, 2 * d)),
        ((0, 2 * d, 7, 0), (2 * d, n, 1, 0), (n + 2 * d, n - 2 * d, 7, 2 * d), (2 * n, n, 6, 0)),
    )
    taken = [{(2 * row + h, i): 0 for h in range(2) for i in range(n)} for row in range(4)]
    for axis, runs_of in enumerate((x_runs, y_runs)):
        for row, runs in enumerate(runs_of):
            for start, length, slot, chunk in runs:
                for i in range(length):
                    taken[row ^ (1, 2)[axis]][slot, chunk + i] = start + i + d
    plan = []
    for runs_of in (x_runs, y_runs):
        most = max(len(runs) for runs in runs_of)
        table = []
        for row, runs in enumerate(runs_of):
            sent, free, rows = 0, 0, []
            for start, length, slot, chunk in runs:
                ready = [taken[row][slot, chunk + i] for i in range(length)]
                at_once = max([free] + ready)
                stream = max([free] + [when - i for i, when in enumerate(ready)])
                if at_once <= stream or at_once <= start:
                    issue, free = (at_once, 0, 0), at_once
                else:
                    issue, free = (-1, stream, stream + length), stream + length - 1
                rows.append(
                    (start, start + length, slot, chunk - start, sent - start, chunk, sent, length)
                    + issue
                )
                sent += length
            rows += [(0,) * 8 + (-1, 0, 0)] * (most - len(runs))
            table.append((rows, sent))
        plan.append(table)
    return plan


def product(left, right, contract):
    return lax.dot_general(
        left,
        right,
        ((contract[:1], contract[1:]), ((), ())),
        precision=lax.Precision.HIGHEST,
        preferred_element_type=jnp.float32,
    )


def lookup(table, x, y):
    a, b, c, d = table
    return a + (b - a) * x + (c - a) * y + (a + d - b - c) * x * y


def factor(block, work):
    size = block.shape[0]
    rows = lax.broadcasted_iota(jnp.int32, (size, size), 0)
    lanes = lax.broadcasted_iota(jnp.int32, (size, size), 1)
    work[:, :size] = block
    work[:, size:] = jnp.where(rows == lanes, 1.0, 0.0).astype(jnp.float32)
    row_of = lax.broadcasted_iota(jnp.int32, (PANEL, size), 0)

    def wide(value):
        return jnp.concatenate([value, value], axis=-1)

    for start in range(0, size, PANEL):
        groups = (size - start) // PANEL
        columns = [
            jnp.broadcast_to(
                work[start:, start + k : start + k + 1], (size - start, size)
            ).reshape(groups, PANEL, size)
            for k in range(PANEL)
        ]
        panel = work[start : start + PANEL, :]
        rest = work[start + PANEL :, :].reshape(groups - 1, PANEL, 2 * size) if groups > 1 else None
        diagonal = jnp.ones((PANEL, size), jnp.float32)
        for k in range(PANEL):
            head = columns[k][0]
            pivot = jnp.broadcast_to(head[k : k + 1], (PANEL, size))
            inverse = 1.0 / pivot
            diagonal = jnp.where(row_of == k, pivot, diagonal)
            weight = jnp.where(row_of > k, head, 0.0) * inverse
            below = columns[k][1:] * inverse[None] if groups > 1 else None
            for j in range(k + 1, PANEL):
                along = jnp.broadcast_to(columns[j][0][k : k + 1], (PANEL, size))
                top = columns[j][0] - weight * along
                if groups > 1:
                    low = columns[j][1:] - below * along[None]
                    columns[j] = jnp.concatenate([top[None], low], axis=0)
                else:
                    columns[j] = top[None]
            row = jnp.broadcast_to(panel[k : k + 1], (PANEL, 2 * size))
            panel = panel - wide(weight) * row
            if groups > 1:
                rest = rest - wide(below) * row[None]
        work[start : start + PANEL, :] = panel * wide(lax.rsqrt(diagonal))
        if groups > 1:
            work[start + PANEL :, :] = rest.reshape(size - start - PANEL, 2 * size)
        yield


def factored(work):
    size = work.shape[0]
    rows = lax.broadcasted_iota(jnp.int32, (size, size), 0)
    lanes = lax.broadcasted_iota(jnp.int32, (size, size), 1)
    return jnp.where(rows <= lanes, work[:, :size], 0.0), work[:, size:]


def kernel(
    cols,
    lag,
    a_ref,
    om_ref,
    basis_ref,
    projected_ref,
    a32,
    high,
    low,
    om,
    part,
    rs_buf,
    sketch,
    gram,
    gram_in,
    t_own,
    t_in,
    t_sum,
    tr_buf,
    t_all,
    work_a,
    work_b,
    a_sem,
    om_sem,
    ring_send,
    ring_recv,
    rs_send,
    rs_recv,
    ag_send,
    ag_recv,
    g_send,
    g_recv,
    t_send,
    t_recv,
):
    _, chunks, depth, width = om_ref.shape
    own_rows = part.shape[1] // cols
    half = RANK // 2
    front, row, col = lax.axis_index("front"), lax.axis_index("row"), lax.axis_index("col")
    x, y = lax.rem(row, 2), lax.div(row, 2)
    beside = (front, row + 1 - 2 * x, col)
    above = (front, row + 2 - 4 * y, col)

    def along(step):
        return (front, row, lax.rem(col + step, cols))

    upper = lax.div(2 * col, cols)
    outward = [step + upper * (cols - 2 * step) for step in range(cols - 1, 0, -1)]

    own_load = pltpu.make_async_copy(om_ref, om.at[pl.ds(2 * row, 2)], om_sem)
    own_load.start()

    def a_load(j):
        columns = pl.ds(pl.multiple_of(j * depth, depth), depth)
        return pltpu.make_async_copy(a_ref.at[:, columns], a32.at[j], a_sem.at[j])

    for i in range(chunks):
        for h in range(2):
            a_load(h * chunks + i).start()

    barrier = pltpu.get_barrier_semaphore()
    peers = [beside, above] + [along(step) for step in range(1, cols)]
    for peer in peers:
        pl.semaphore_signal(barrier, inc=1, device_id=peer, device_id_type=MESH)
    part[...] = jnp.zeros_like(part)
    own_load.wait()
    pl.semaphore_wait(barrier, len(peers))

    plan = send_plan(chunks, lag)
    total_steps = 3 * chunks + lag

    def runs_at(axis, px, py):
        table = plan[axis]
        return [
            [lookup([rows[k][field] for rows, _ in table], px, py) for field in range(11)]
            for k in range(len(table[0][0]))
        ]

    leaving = [runs_at(axis, x, y) for axis in (0, 1)]
    coming = [runs_at(0, 1 - x, y), runs_at(1, x, 1 - y)]

    def chosen(runs, at):
        live, slot, i, order = False, 0, 0, 0
        for start, end, run_slot, run_chunk, run_order, *_ in runs:
            inside = jnp.logical_and(at >= start, at < end)
            live = jnp.logical_or(live, inside)
            slot = jnp.where(inside, run_slot, slot)
            i = jnp.where(inside, run_chunk + at, i)
            order = jnp.where(inside, run_order + at, order)
        return live, slot, i, order

    def hop(axis, slot, i, order):
        return pltpu.make_async_remote_copy(
            src_ref=om.at[slot, i],
            dst_ref=om.at[slot, i],
            send_sem=ring_send.at[axis, order],
            recv_sem=ring_recv.at[axis, order],
            device_id=(beside, above)[axis],
            device_id_type=MESH,
        )

    def accumulate(slot, i):
        block = lax.div(slot, 2)
        j = lax.rem(slot, 2) * chunks + i
        columns = om[slot, i]
        part[block] += jnp.dot(
            high[j], columns, preferred_element_type=jnp.float32
        ) + jnp.dot(low[j], columns, preferred_element_type=jnp.float32)

    def issue(axis, g):
        for k, run in enumerate(leaving[axis]):
            _, _, slot, _, _, chunk, sent, length, at_once, stream, stop = run
            if any(rows[k][8] >= 0 for rows, _ in plan[axis]):

                @pl.when(at_once == g)
                def _():
                    @pl.loop(0, length)
                    def _(i):
                        hop(axis, slot, chunk + i, sent + i).start()

            if any(rows[k][10] > 0 for rows, _ in plan[axis]):

                @pl.when(jnp.logical_and(g >= stream, g < stop))
                def _():
                    i = g - stream
                    hop(axis, slot, chunk + i, sent + i).start()

    def step_of(g, convert):
        found = []
        for axis in (0, 1):
            live, slot, i, order = chosen(coming[axis], g - lag)
            found.append((live, slot, i))

            @pl.when(live)
            def _():
                hop(axis, slot, i, order).wait_recv()

            issue(1 - axis, g)

        if convert:
            for h in range(2):
                j = h * chunks + g
                a_load(j).wait()
                value = a32[j]
                near = value.astype(jnp.bfloat16)
                high[j] = near
                low[j] = (value - near.astype(jnp.float32)).astype(jnp.bfloat16)
            for h in range(2):
                accumulate(2 * row + h, g)
        for live, slot, i in found:

            @pl.when(live)
            def _():
                accumulate(slot, i)

    def gather(hooks):
        marks = sorted(set(hooks) | {chunks, total_steps})
        begin = 0
        for mark in marks:
            if mark > begin + 1:
                pl.loop(begin, mark)(functools.partial(step_of, convert=mark <= chunks))
            elif mark > begin:
                step_of(begin, convert=mark <= chunks)
            for hook in hooks.get(mark, ()):
                hook()
            begin = mark

    def scatter(s, step):
        target = lax.rem(col + step, cols)
        rows = pl.ds(pl.multiple_of(target * own_rows, own_rows), own_rows)
        return pltpu.make_async_remote_copy(
            src_ref=part.at[s, rows],
            dst_ref=rs_buf.at[s, step - 1],
            send_sem=rs_send.at[s, step - 1],
            recv_sem=rs_recv.at[s, step - 1],
            device_id=along(step),
            device_id_type=MESH,
        )

    def spread(s, step, piece):
        return pltpu.make_async_remote_copy(
            src_ref=sketch.at[s, piece],
            dst_ref=sketch.at[s, piece],
            send_sem=ag_send.at[s, step - 1],
            recv_sem=ag_recv.at[s, step - 1],
            device_id=along(step),
            device_id_type=MESH,
        )

    def scatter_start(s):
        for step in outward:
            scatter(s, step).start()

    def scatter_end(s):
        rows = pl.ds(pl.multiple_of(col * own_rows, own_rows), own_rows)
        total = part[s, rows]
        for step in range(1, cols):
            scatter(s, step).wait_recv()
            total = total + rs_buf[s, step - 1]
        sketch[s, col] = total
        for step in outward:
            spread(s, step, col).start()

    def spread_end(s):
        for step in range(1, cols):
            spread(s, step, lax.rem(col + cols - step, cols)).wait_recv()
        return sketch[s].reshape(part.shape[1], width)

    def exchange(first, count):
        return pltpu.make_async_remote_copy(
            src_ref=gram.at[pl.ds(first, count)],
            dst_ref=gram_in.at[pl.ds(first, count)],
            send_sem=g_send.at[first],
            recv_sem=g_recv.at[first],
            device_id=beside,
            device_id_type=MESH,
        )

    factor_a = []

    def first_done():
        value = spread_end(0)
        gram[0] = product(value, value, (0, 0))
        exchange(0, 1).start()

    def first_panel():
        exchange(0, 1).wait_recv()
        factor_a.append(factor(gram[0] + gram_in[0], work_a))
        next(factor_a[0])

    def next_panel():
        for _ in range(PANELS_A_STEP):
            next(factor_a[0], None)

    ready = chunks + 3 * lag
    ready_next = 2 * chunks + 2 * lag
    panels = half // PANEL
    panel_step = min(ready + 2 * SUM_LAG + FACTOR_LAG, total_steps)
    hooks = {}
    for at, hook in (
        (ready, lambda: scatter_start(0)),
        (ready + SUM_LAG, lambda: scatter_end(0)),
        (ready_next, lambda: scatter_start(1)),
        (ready + 2 * SUM_LAG, first_done),
        (ready_next + SUM_LAG, lambda: scatter_end(1)),
        (panel_step, first_panel),
    ):
        hooks.setdefault(min(at, total_steps), []).append(hook)
    for at in range(panel_step + 1, total_steps + 1):
        hooks.setdefault(at, []).append(next_panel)
    gather(hooks)
    for _ in factor_a[0]:
        pass

    first = sketch[0].reshape(part.shape[1], width)
    upper_a, inverse_a = factored(work_a)
    q_a = product(first, inverse_a, (1, 1))

    def projection(left):
        return jnp.concatenate(
            [product(left, part[2 + s], (0, 0)) for s in range(2)], axis=1
        )

    t_own[0] = projection(q_a)
    second = spread_end(1)
    gram[1] = product(first, second, (0, 0))
    exchange(1, 1).start()
    gram[2] = product(second, second, (0, 0))
    exchange(2, 1).start()
    coarse = projection(second)
    mine_a = product(sketch[0, col], inverse_a, (1, 1))
    basis_ref[:, :half] = mine_a
    exchange(1, 1).wait_recv()
    across = product(inverse_a, gram[1] + gram_in[1], (1, 0))
    t_own[1] = coarse - product(across, t_own[0], (0, 0))

    swap = pltpu.make_async_remote_copy(
        src_ref=t_own.at[1 - x],
        dst_ref=t_in,
        send_sem=t_send.at[0, 0],
        recv_sem=t_recv.at[0, 0],
        device_id=beside,
        device_id_type=MESH,
    )
    swap.start()
    exchange(2, 1).wait_recv()
    schur = gram[2] + gram_in[2] - product(across, across, (0, 0))
    factor_b = factor(schur, work_b)
    for _ in factor_b:
        pass
    swap.wait_recv()
    t_sum[...] = (t_own[x] + t_in[...]).reshape(t_sum.shape)

    def t_scatter(step):
        return pltpu.make_async_remote_copy(
            src_ref=t_sum.at[lax.rem(col + step, cols)],
            dst_ref=tr_buf.at[step - 1],
            send_sem=t_send.at[1, step - 1],
            recv_sem=t_recv.at[1, step - 1],
            device_id=along(step),
            device_id_type=MESH,
        )

    def t_spread(step, piece):
        return pltpu.make_async_remote_copy(
            src_ref=t_all.at[piece],
            dst_ref=t_all.at[piece],
            send_sem=t_send.at[2, step - 1],
            recv_sem=t_recv.at[2, step - 1],
            device_id=along(step),
            device_id_type=MESH,
        )

    for step in outward:
        t_scatter(step).start()
    upper_b, inverse_b = factored(work_b)
    mine_b = sketch[1, col] - product(mine_a, across, (1, 0))
    basis_ref[:, half:] = product(mine_b, inverse_b, (1, 1))
    total = t_sum[col]
    for step in range(1, cols):
        t_scatter(step).wait_recv()
        total = total + tr_buf[step - 1]
    t_all[col] = total
    for step in outward:
        t_spread(step, col).start()

    for step in range(1, cols):
        t_spread(step, lax.rem(col + cols - step, cols)).wait_recv()
    tail = t_all[...].reshape(half, 2 * width)
    is_low = x == 0
    projected_ref[:, :half] = jnp.where(is_low, upper_a, 0.0)
    projected_ref[:, half:RANK] = jnp.where(is_low, across, upper_b)
    projected_ref[:, RANK:] = jnp.where(is_low, tail, product(inverse_b, tail, (1, 0)))

    for axis in (0, 1):

        @pl.loop(0, lookup([sent for _, sent in plan[axis]], x, y))
        def _(order):
            hop(axis, 0, 0, order).wait_send()

    for step in range(1, cols):
        for s in range(2):
            scatter(s, step).wait_send()
            spread(s, step, col).wait_send()
        t_scatter(step).wait_send()
        t_spread(step, col).wait_send()
    exchange(0, 1).wait_send()
    exchange(1, 1).wait_send()
    exchange(2, 1).wait_send()
    swap.wait_send()


def per_device(front_rows, random_columns):
    block_rows, depth = front_rows.shape
    width = random_columns.shape[1]
    cols = lax.axis_size("col")
    half = RANK // 2
    own_rows = block_rows // cols
    chunk = min(CHUNK, depth // 12 // 128 * 128)
    chunks = depth // 2 // chunk
    lag = max(1, min(LAG, chunks // 4))
    columns = random_columns.reshape(2, chunks, chunk, width)
    vmem = pltpu.VMEM
    f32, bf16 = jnp.float32, jnp.bfloat16
    dma = pltpu.SemaphoreType.DMA
    return pl.pallas_call(
        functools.partial(kernel, cols, lag),
        out_shape=(
            jax.ShapeDtypeStruct((own_rows, RANK), f32),
            jax.ShapeDtypeStruct((half, 4 * width), f32),
        ),
        in_specs=[pl.BlockSpec(memory_space=pl.ANY)] * 2,
        out_specs=(pl.BlockSpec(memory_space=pltpu.VMEM),) * 2,
        scratch_shapes=[
            vmem((2 * chunks, block_rows, chunk), f32),
            vmem((2 * chunks, block_rows, chunk), bf16),
            vmem((2 * chunks, block_rows, chunk), bf16),
            vmem((8, chunks, chunk, width), bf16),
            vmem((4, block_rows, width), f32),
            vmem((2, cols - 1, own_rows, width), f32),
            vmem((2, cols, own_rows, width), f32),
            vmem((3, half, half), f32),
            vmem((3, half, half), f32),
            vmem((2, half, 2 * width), f32),
            vmem((half, 2 * width), f32),
            vmem((cols, half // cols, 2 * width), f32),
            vmem((cols - 1, half // cols, 2 * width), f32),
            vmem((cols, half // cols, 2 * width), f32),
            vmem((half, RANK), f32),
            vmem((half, RANK), f32),
            dma((2 * chunks,)),
            dma,
            dma((2, 3 * chunks + lag)),
            dma((2, 3 * chunks + lag)),
            dma((2, cols - 1)),
            dma((2, cols - 1)),
            dma((2, cols - 1)),
            dma((2, cols - 1)),
            dma((3,)),
            dma((3,)),
            dma((3, cols - 1)),
            dma((3, cols - 1)),
        ],
        compiler_params=pltpu.CompilerParams(
            collective_id=0, has_side_effects=True, vmem_limit_bytes=60 << 20
        ),
    )(front_rows, columns)


def solution(mesh):
    return jax.shard_map(
        per_device,
        mesh=mesh,
        in_specs=(P(("front", "row"), "col"), P(("front", "col"), "row")),
        out_specs=(P(("front", "row", "col"), None), P(("front", "row"), None)),
        check_vma=False,
    )
```

```python
import functools

import jax
import jax.numpy as jnp
from jax import lax
from jax.experimental import pallas as pl
from jax.experimental.pallas import tpu as pltpu
from jax.sharding import PartitionSpec as P

RANK = 256
PANEL = 8
CHUNK = 256
LAG = 3
SUM_LAG = 6
FACTOR_LAG = 9
PANELS_A_STEP = 4
MESH = pl.DeviceIdType.MESH


def send_plan(size, lag):
    n, d = size, lag
    x_runs = (
        ((0, n, 0, 0), (n, n, 5, 0), (2 * n, n, 4, 0)),
        ((0, n, 2, 0), (n, n, 3, 0), (2 * n, n, 7, 0)),
        ((0, d, 4, 0), (d, n, 1, 0), (n + d, n, 2, 0), (2 * n + d, n - d, 4, d)),
        (
            (0, 2 * d, 6, 0),
            (2 * d, n, 0, 0),
            (n + 2 * d, n - d, 3, 0),
            (2 * n + d, n - 2 * d, 6, 2 * d),
            (3 * n - d, d, 7, n - d),
        ),
    )
    y_runs = (
        ((0, n, 1, 0), (n, n, 2, 0), (2 * n, d, 3, n - d), (2 * n + d, n - d, 7, 0)),
        ((0, d, 3, 0), (d, n, 0, 0), (n + d, n - d, 3, d), (2 * n, n, 5, 0)),
        ((0, n, 5, 0), (n, n, 4, 0), (2 * n, 2 * d, 6, 0), (2 * n + 2 * d, n - 2 * d, 6, 2 * d)),
        ((0, 2 * d, 7, 0), (2 * d, n, 1, 0), (n + 2 * d, n - 2 * d, 7, 2 * d), (2 * n, n, 6, 0)),
    )
    taken = [{(2 * row + h, i): 0 for h in range(2) for i in range(n)} for row in range(4)]
    for axis, runs_of in enumerate((x_runs, y_runs)):
        for row, runs in enumerate(runs_of):
            for start, length, slot, chunk in runs:
                for i in range(length):
                    taken[row ^ (1, 2)[axis]][slot, chunk + i] = start + i + d
    plan = []
    for runs_of in (x_runs, y_runs):
        most = max(len(runs) for runs in runs_of)
        table = []
        for row, runs in enumerate(runs_of):
            sent, free, rows = 0, 0, []
            for start, length, slot, chunk in runs:
                ready = [taken[row][slot, chunk + i] for i in range(length)]
                at_once = max([free] + ready)
                stream = max([free] + [when - i for i, when in enumerate(ready)])
                if at_once <= stream or at_once <= start:
                    issue, free = (at_once, 0, 0), at_once
                else:
                    issue, free = (-1, stream, stream + length), stream + length - 1
                rows.append(
                    (start, start + length, slot, chunk - start, sent - start, chunk, sent, length)
                    + issue
                )
                sent += length
            rows += [(0,) * 8 + (-1, 0, 0)] * (most - len(runs))
            table.append((rows, sent))
        plan.append(table)
    return plan


def product(left, right, contract):
    return lax.dot_general(
        left,
        right,
        ((contract[:1], contract[1:]), ((), ())),
        precision=lax.Precision.HIGHEST,
        preferred_element_type=jnp.float32,
    )


def lookup(table, x, y):
    a, b, c, d = table
    return a + (b - a) * x + (c - a) * y + (a + d - b - c) * x * y


def factor(block, work):
    size = block.shape[0]
    rows = lax.broadcasted_iota(jnp.int32, (size, size), 0)
    lanes = lax.broadcasted_iota(jnp.int32, (size, size), 1)
    work[:, :size] = block
    work[:, size:] = jnp.where(rows == lanes, 1.0, 0.0).astype(jnp.float32)
    row_of = lax.broadcasted_iota(jnp.int32, (PANEL, size), 0)

    def wide(value):
        return jnp.concatenate([value, value], axis=-1)

    for start in range(0, size, PANEL):
        groups = (size - start) // PANEL
        columns = [
            jnp.broadcast_to(
                work[start:, start + k : start + k + 1], (size - start, size)
            ).reshape(groups, PANEL, size)
            for k in range(PANEL)
        ]
        panel = work[start : start + PANEL, :]
        rest = work[start + PANEL :, :].reshape(groups - 1, PANEL, 2 * size) if groups > 1 else None
        diagonal = jnp.ones((PANEL, size), jnp.float32)
        for k in range(PANEL):
            head = columns[k][0]
            pivot = jnp.broadcast_to(head[k : k + 1], (PANEL, size))
            inverse = 1.0 / pivot
            diagonal = jnp.where(row_of == k, pivot, diagonal)
            weight = jnp.where(row_of > k, head, 0.0) * inverse
            below = columns[k][1:] * inverse[None] if groups > 1 else None
            for j in range(k + 1, PANEL):
                along = jnp.broadcast_to(columns[j][0][k : k + 1], (PANEL, size))
                top = columns[j][0] - weight * along
                if groups > 1:
                    low = columns[j][1:] - below * along[None]
                    columns[j] = jnp.concatenate([top[None], low], axis=0)
                else:
                    columns[j] = top[None]
            row = jnp.broadcast_to(panel[k : k + 1], (PANEL, 2 * size))
            panel = panel - wide(weight) * row
            if groups > 1:
                rest = rest - wide(below) * row[None]
        work[start : start + PANEL, :] = panel * wide(lax.rsqrt(diagonal))
        if groups > 1:
            work[start + PANEL :, :] = rest.reshape(size - start - PANEL, 2 * size)
        yield


def factored(work):
    size = work.shape[0]
    rows = lax.broadcasted_iota(jnp.int32, (size, size), 0)
    lanes = lax.broadcasted_iota(jnp.int32, (size, size), 1)
    return jnp.where(rows <= lanes, work[:, :size], 0.0), work[:, size:]


def kernel(
    cols,
    lag,
    a_ref,
    om_ref,
    basis_ref,
    projected_ref,
    a32,
    high,
    low,
    om,
    part,
    rs_buf,
    sketch,
    gram,
    gram_in,
    t_own,
    t_in,
    t_sum,
    tr_buf,
    t_all,
    work_a,
    work_b,
    a_sem,
    om_sem,
    ring_send,
    ring_recv,
    rs_send,
    rs_recv,
    ag_send,
    ag_recv,
    g_send,
    g_recv,
    t_send,
    t_recv,
):
    _, chunks, depth, width = om_ref.shape
    own_rows = part.shape[1] // cols
    half = RANK // 2
    front, row, col = lax.axis_index("front"), lax.axis_index("row"), lax.axis_index("col")
    x, y = lax.rem(row, 2), lax.div(row, 2)
    beside = (front, row + 1 - 2 * x, col)
    above = (front, row + 2 - 4 * y, col)

    def along(step):
        return (front, row, lax.rem(col + step, cols))

    upper = lax.div(2 * col, cols)
    outward = [step + upper * (cols - 2 * step) for step in range(cols - 1, 0, -1)]

    own_load = pltpu.make_async_copy(om_ref, om.at[pl.ds(2 * row, 2)], om_sem)
    own_load.start()

    def a_load(j):
        columns = pl.ds(pl.multiple_of(j * depth, depth), depth)
        return pltpu.make_async_copy(a_ref.at[:, columns], a32.at[j], a_sem.at[j])

    for i in range(chunks):
        for h in range(2):
            a_load(h * chunks + i).start()

    barrier = pltpu.get_barrier_semaphore()
    peers = [beside, above] + [along(step) for step in range(1, cols)]
    for peer in peers:
        pl.semaphore_signal(barrier, inc=1, device_id=peer, device_id_type=MESH)
    part[...] = jnp.zeros_like(part)
    own_load.wait()
    pl.semaphore_wait(barrier, len(peers))

    plan = send_plan(chunks, lag)
    total_steps = 3 * chunks + lag

    def runs_at(axis, px, py):
        table = plan[axis]
        return [
            [lookup([rows[k][field] for rows, _ in table], px, py) for field in range(11)]
            for k in range(len(table[0][0]))
        ]

    leaving = [runs_at(axis, x, y) for axis in (0, 1)]
    coming = [runs_at(0, 1 - x, y), runs_at(1, x, 1 - y)]

    def chosen(runs, at):
        live, slot, i, order = False, 0, 0, 0
        for start, end, run_slot, run_chunk, run_order, *_ in runs:
            inside = jnp.logical_and(at >= start, at < end)
            live = jnp.logical_or(live, inside)
            slot = jnp.where(inside, run_slot, slot)
            i = jnp.where(inside, run_chunk + at, i)
            order = jnp.where(inside, run_order + at, order)
        return live, slot, i, order

    def hop(axis, slot, i, order):
        return pltpu.make_async_remote_copy(
            src_ref=om.at[slot, i],
            dst_ref=om.at[slot, i],
            send_sem=ring_send.at[axis, order],
            recv_sem=ring_recv.at[axis, order],
            device_id=(beside, above)[axis],
            device_id_type=MESH,
        )

    def accumulate(slot, i):
        block = lax.div(slot, 2)
        j = lax.rem(slot, 2) * chunks + i
        columns = om[slot, i]
        part[block] += jnp.dot(
            high[j], columns, preferred_element_type=jnp.float32
        ) + jnp.dot(low[j], columns, preferred_element_type=jnp.float32)

    def issue(axis, g):
        for k, run in enumerate(leaving[axis]):
            _, _, slot, _, _, chunk, sent, length, at_once, stream, stop = run
            if any(rows[k][8] >= 0 for rows, _ in plan[axis]):

                @pl.when(at_once == g)
                def _():
                    @pl.loop(0, length)
                    def _(i):
                        hop(axis, slot, chunk + i, sent + i).start()

            if any(rows[k][10] > 0 for rows, _ in plan[axis]):

                @pl.when(jnp.logical_and(g >= stream, g < stop))
                def _():
                    i = g - stream
                    hop(axis, slot, chunk + i, sent + i).start()

    def step_of(g, convert):
        found = []
        for axis in (0, 1):
            live, slot, i, order = chosen(coming[axis], g - lag)
            found.append((live, slot, i))

            @pl.when(live)
            def _():
                hop(axis, slot, i, order).wait_recv()

            issue(1 - axis, g)

        if convert:
            for h in range(2):
                j = h * chunks + g
                a_load(j).wait()
                value = a32[j]
                near = value.astype(jnp.bfloat16)
                high[j] = near
                low[j] = (value - near.astype(jnp.float32)).astype(jnp.bfloat16)
            for h in range(2):
                accumulate(2 * row + h, g)
        for live, slot, i in found:

            @pl.when(live)
            def _():
                accumulate(slot, i)

    def gather(hooks):
        marks = sorted(set(hooks) | {chunks, total_steps})
        begin = 0
        for mark in marks:
            if mark > begin + 1:
                pl.loop(begin, mark)(functools.partial(step_of, convert=mark <= chunks))
            elif mark > begin:
                step_of(begin, convert=mark <= chunks)
            for hook in hooks.get(mark, ()):
                hook()
            begin = mark

    def scatter(s, step):
        target = lax.rem(col + step, cols)
        rows = pl.ds(pl.multiple_of(target * own_rows, own_rows), own_rows)
        return pltpu.make_async_remote_copy(
            src_ref=part.at[s, rows],
            dst_ref=rs_buf.at[s, step - 1],
            send_sem=rs_send.at[s, step - 1],
            recv_sem=rs_recv.at[s, step - 1],
            device_id=along(step),
            device_id_type=MESH,
        )

    def spread(s, step, piece):
        return pltpu.make_async_remote_copy(
            src_ref=sketch.at[s, piece],
            dst_ref=sketch.at[s, piece],
            send_sem=ag_send.at[s, step - 1],
            recv_sem=ag_recv.at[s, step - 1],
            device_id=along(step),
            device_id_type=MESH,
        )

    def scatter_start(s):
        for step in outward:
            scatter(s, step).start()

    def scatter_end(s):
        rows = pl.ds(pl.multiple_of(col * own_rows, own_rows), own_rows)
        total = part[s, rows]
        for step in range(1, cols):
            scatter(s, step).wait_recv()
            total = total + rs_buf[s, step - 1]
        sketch[s, col] = total
        for step in outward:
            spread(s, step, col).start()

    def spread_end(s):
        for step in range(1, cols):
            spread(s, step, lax.rem(col + cols - step, cols)).wait_recv()
        return sketch[s].reshape(part.shape[1], width)

    def exchange(first, count):
        return pltpu.make_async_remote_copy(
            src_ref=gram.at[pl.ds(first, count)],
            dst_ref=gram_in.at[pl.ds(first, count)],
            send_sem=g_send.at[first],
            recv_sem=g_recv.at[first],
            device_id=beside,
            device_id_type=MESH,
        )

    factor_a = []

    def first_done():
        value = spread_end(0)
        gram[0] = product(value, value, (0, 0))
        exchange(0, 1).start()

    def first_panel():
        exchange(0, 1).wait_recv()
        factor_a.append(factor(gram[0] + gram_in[0], work_a))
        next(factor_a[0])

    def next_panel():
        for _ in range(PANELS_A_STEP):
            next(factor_a[0], None)

    ready = chunks + 3 * lag
    ready_next = 2 * chunks + 2 * lag
    panels = half // PANEL
    panel_step = min(ready + 2 * SUM_LAG + FACTOR_LAG, total_steps)
    hooks = {}
    for at, hook in (
        (ready, lambda: scatter_start(0)),
        (ready + SUM_LAG, lambda: scatter_end(0)),
        (ready_next, lambda: scatter_start(1)),
        (ready + 2 * SUM_LAG, first_done),
        (ready_next + SUM_LAG - 1, lambda: scatter_end(1)),
        (panel_step, first_panel),
    ):
        hooks.setdefault(min(at, total_steps), []).append(hook)
    for at in range(panel_step + 1, total_steps + 1):
        hooks.setdefault(at, []).append(next_panel)
    gather(hooks)
    for _ in factor_a[0]:
        pass

    first = sketch[0].reshape(part.shape[1], width)
    upper_a, inverse_a = factored(work_a)
    q_a = product(first, inverse_a, (1, 1))

    def projection(left):
        return jnp.concatenate(
            [product(left, part[2 + s], (0, 0)) for s in range(2)], axis=1
        )

    t_own[0] = projection(q_a)
    second = spread_end(1)
    gram[1] = product(first, second, (0, 0))
    exchange(1, 1).start()
    gram[2] = product(second, second, (0, 0))
    exchange(2, 1).start()
    coarse = projection(second)
    mine_a = product(sketch[0, col], inverse_a, (1, 1))
    basis_ref[:, :half] = mine_a
    exchange(1, 1).wait_recv()
    across = product(inverse_a, gram[1] + gram_in[1], (1, 0))
    t_own[1] = coarse - product(across, t_own[0], (0, 0))

    swap = pltpu.make_async_remote_copy(
        src_ref=t_own.at[1 - x],
        dst_ref=t_in,
        send_sem=t_send.at[0, 0],
        recv_sem=t_recv.at[0, 0],
        device_id=beside,
        device_id_type=MESH,
    )
    swap.start()
    exchange(2, 1).wait_recv()
    schur = gram[2] + gram_in[2] - product(across, across, (0, 0))
    factor_b = factor(schur, work_b)
    for _ in factor_b:
        pass
    swap.wait_recv()
    t_sum[...] = (t_own[x] + t_in[...]).reshape(t_sum.shape)

    def t_scatter(step):
        return pltpu.make_async_remote_copy(
            src_ref=t_sum.at[lax.rem(col + step, cols)],
            dst_ref=tr_buf.at[step - 1],
            send_sem=t_send.at[1, step - 1],
            recv_sem=t_recv.at[1, step - 1],
            device_id=along(step),
            device_id_type=MESH,
        )

    def t_spread(step, piece):
        return pltpu.make_async_remote_copy(
            src_ref=t_all.at[piece],
            dst_ref=t_all.at[piece],
            send_sem=t_send.at[2, step - 1],
            recv_sem=t_recv.at[2, step - 1],
            device_id=along(step),
            device_id_type=MESH,
        )

    for step in outward:
        t_scatter(step).start()
    upper_b, inverse_b = factored(work_b)
    mine_b = sketch[1, col] - product(mine_a, across, (1, 0))
    basis_ref[:, half:] = product(mine_b, inverse_b, (1, 1))
    total = t_sum[col]
    for step in range(1, cols):
        t_scatter(step).wait_recv()
        total = total + tr_buf[step - 1]
    t_all[col] = total
    for step in outward:
        t_spread(step, col).start()

    for step in range(1, cols):
        t_spread(step, lax.rem(col + cols - step, cols)).wait_recv()
    tail = t_all[...].reshape(half, 2 * width)
    is_low = x == 0
    projected_ref[:, :half] = jnp.where(is_low, upper_a, 0.0)
    projected_ref[:, half:RANK] = jnp.where(is_low, across, upper_b)
    projected_ref[:, RANK:] = jnp.where(is_low, tail, product(inverse_b, tail, (1, 0)))

    for axis in (0, 1):

        @pl.loop(0, lookup([sent for _, sent in plan[axis]], x, y))
        def _(order):
            hop(axis, 0, 0, order).wait_send()

    for step in range(1, cols):
        for s in range(2):
            scatter(s, step).wait_send()
            spread(s, step, col).wait_send()
        t_scatter(step).wait_send()
        t_spread(step, col).wait_send()
    exchange(0, 1).wait_send()
    exchange(1, 1).wait_send()
    exchange(2, 1).wait_send()
    swap.wait_send()


def per_device(front_rows, random_columns):
    block_rows, depth = front_rows.shape
    width = random_columns.shape[1]
    cols = lax.axis_size("col")
    half = RANK // 2
    own_rows = block_rows // cols
    chunk = min(CHUNK, depth // 12 // 128 * 128)
    chunks = depth // 2 // chunk
    lag = max(1, min(LAG, chunks // 4))
    columns = random_columns.reshape(2, chunks, chunk, width)
    vmem = pltpu.VMEM
    f32, bf16 = jnp.float32, jnp.bfloat16
    dma = pltpu.SemaphoreType.DMA
    return pl.pallas_call(
        functools.partial(kernel, cols, lag),
        out_shape=(
            jax.ShapeDtypeStruct((own_rows, RANK), f32),
            jax.ShapeDtypeStruct((half, 4 * width), f32),
        ),
        in_specs=[pl.BlockSpec(memory_space=pl.ANY)] * 2,
        out_specs=(pl.BlockSpec(memory_space=pltpu.VMEM),) * 2,
        scratch_shapes=[
            vmem((2 * chunks, block_rows, chunk), f32),
            vmem((2 * chunks, block_rows, chunk), bf16),
            vmem((2 * chunks, block_rows, chunk), bf16),
            vmem((8, chunks, chunk, width), bf16),
            vmem((4, block_rows, width), f32),
            vmem((2, cols - 1, own_rows, width), f32),
            vmem((2, cols, own_rows, width), f32),
            vmem((3, half, half), f32),
            vmem((3, half, half), f32),
            vmem((2, half, 2 * width), f32),
            vmem((half, 2 * width), f32),
            vmem((cols, half // cols, 2 * width), f32),
            vmem((cols - 1, half // cols, 2 * width), f32),
            vmem((cols, half // cols, 2 * width), f32),
            vmem((half, RANK), f32),
            vmem((half, RANK), f32),
            dma((2 * chunks,)),
            dma,
            dma((2, 3 * chunks + lag)),
            dma((2, 3 * chunks + lag)),
            dma((2, cols - 1)),
            dma((2, cols - 1)),
            dma((2, cols - 1)),
            dma((2, cols - 1)),
            dma((3,)),
            dma((3,)),
            dma((3, cols - 1)),
            dma((3, cols - 1)),
        ],
        compiler_params=pltpu.CompilerParams(
            collective_id=0, has_side_effects=True, vmem_limit_bytes=60 << 20
        ),
    )(front_rows, columns)


def solution(mesh):
    return jax.shard_map(
        per_device,
        mesh=mesh,
        in_specs=(P(("front", "row"), "col"), P(("front", "col"), "row")),
        out_specs=(P(("front", "row", "col"), None), P(("front", "row"), None)),
        check_vma=False,
    )
```
